32 devices in a mesh: ta: 8 (over y, x, core), ga: 4 (over z).
Axes of the slice: x: 2, y: 2, z: 4, core: 2. Of those that a mesh axis runs over, the one named last changes fastest.
Arguments:
- snapshots: bfloat16 [1024, 4, 16384], P('ta', 'ga'), may hold values from -12 to 12
- block_starts: int32 [7], replicated, may hold values from 0 to 768
- kept_freqs: int32 [32], replicated, may hold values from 0 to 128
Outputs:
- spectra: bfloat16 [4, 7, 2, 32, 16384], P('ga', None, None, None, 'ta')
- power_step: float32 [4, 7, 2, 32, 16384], P('ga', None, None, None, 'ta')
The draws below stay inside these ranges and needn't reach their ends.
All inputs are finite; a program needn't handle non-finite values.
Results may differ from the reference program's by a relative error of at most 0.0047.
Values may be sent and summed in bfloat16 or wider, within the bound.
A program may use at most 192 MiB of HBM per device.

```python
import math
import jax
import jax.numpy as jnp
from jax import lax

NT = 1024
NFFT = 256
NB = 7
NF = 32
GROUPS = 4
GROUP_PTS = 16384


def draw_snapshots(key, part):
    key_noise = jax.random.fold_in(key, 11)
    key_rough = jax.random.fold_in(key, 12)
    total_pts = GROUPS * GROUP_PTS
    position = jnp.arange(total_pts, dtype=jnp.float32) / (total_pts - 1)
    roughness = jax.random.uniform(key_rough, (total_pts,), jnp.float32, 0.7, 1.4)
    amplitude = roughness * jnp.exp(position * (0.5 * math.log(3.0)))
    values = amplitude[None, :] * jax.random.normal(key_noise, (NT, total_pts), jnp.float32)
    values = jnp.clip(values, -12.0, 12.0)
    return values.reshape(NT, GROUPS, GROUP_PTS).astype(jnp.bfloat16)


def with_ends(entries, rng, low, largest):
    place = [jax.random.randint(jax.random.fold_in(rng, axis), (), 0, length) for axis, length in enumerate(entries.shape)]
    main_axis = entries.shape.index(max(entries.shape))
    neighbour = place[:main_axis] + [(place[main_axis] + 1) % entries.shape[main_axis]] + place[main_axis + 1:]
    return entries.at[tuple(place)].set(low).at[tuple(neighbour)].set(largest)


def setup_inputs(seed: int = 0) -> dict:
    streams_of = jax.random.split(jax.random.key(seed), 4)
    snapshots = draw_snapshots(jax.random.fold_in(streams_of[3], 71), 0)
    block_starts = with_ends(jax.random.randint(streams_of[1], (NB,), 0, NT - NFFT + 1), jax.random.fold_in(streams_of[1], 1), 0, NT - NFFT).astype(jnp.int32)
    kept_freqs = with_ends(jax.random.randint(streams_of[2], (NF,), 0, NFFT // 2 + 1), jax.random.fold_in(streams_of[2], 1), 0, (NFFT // 2 + 1) - 1).astype(jnp.int32)
    return {"snapshots": snapshots, "block_starts": block_starts, "kept_freqs": kept_freqs}


def kernel_table(kept_freqs, sample_index):
    phase_index = kept_freqs[:, None] * sample_index[None, :] % NFFT
    angle_val = 2.0 * math.pi / NFFT * phase_index.astype(jnp.float32)
    window = 0.5 - 0.5 * jnp.cos(2.0 * math.pi / NFFT * sample_index.astype(jnp.float32))
    norm_scale = 2.0 / math.sqrt(NFFT)
    real_rows = window[None, :] * jnp.cos(angle_val) * norm_scale
    imag_rows = -window[None, :] * jnp.sin(angle_val) * norm_scale
    return jnp.concatenate([real_rows, imag_rows], axis=0)

def reference(snapshots, block_starts, kept_freqs):
    total_pts = GROUPS * GROUP_PTS
    series = snapshots.reshape(NT, total_pts)
    kernel_rows = kernel_table(kept_freqs, jnp.arange(NFFT, dtype=jnp.int32)).astype(jnp.bfloat16)
    blocks = []
    for block_index in range(NB):
        segment = lax.dynamic_slice_in_dim(series, block_starts[block_index].astype(jnp.int32), NFFT, 0)
        blocks.append(jnp.dot(kernel_rows, segment, preferred_element_type=jnp.float32).astype(jnp.bfloat16))
    spectra = jnp.stack(blocks)
    values = spectra.astype(jnp.float32).reshape(NB, 2, NF, total_pts)
    real_part = values[:, 0]
    imag_part = values[:, 1]
    highest = lax.Precision.HIGHEST
    denominator = float(NB * total_pts)
    gram_re = (jnp.einsum('bfp,cfp->fbc', real_part, real_part, precision=highest) + jnp.einsum('bfp,cfp->fbc', imag_part, imag_part, precision=highest)) / denominator
    gram_im = (jnp.einsum('bfp,cfp->fbc', real_part, imag_part, precision=highest) - jnp.einsum('bfp,cfp->fbc', imag_part, real_part, precision=highest)) / denominator
    out_re = jnp.einsum('cfp,fcb->bfp', real_part, gram_re, precision=highest) - jnp.einsum('cfp,fcb->bfp', imag_part, gram_im, precision=highest)
    out_im = jnp.einsum('cfp,fcb->bfp', real_part, gram_im, precision=highest) + jnp.einsum('cfp,fcb->bfp', imag_part, gram_re, precision=highest)
    power = jnp.stack([out_re, out_im], axis=1)
    spectra_out = spectra.reshape(NB, 2, NF, GROUPS, GROUP_PTS).transpose(3, 0, 1, 2, 4)
    power_out = power.reshape(NB, 2, NF, GROUPS, GROUP_PTS).transpose(3, 0, 1, 2, 4)
    return (spectra_out, power_out)
```

```python
import functools
import math

import jax
import jax.numpy as jnp
from jax import lax
from jax.experimental import pallas as pl
from jax.experimental.pallas import tpu as pltpu
from jax.sharding import PartitionSpec as P

NFFT = 256
MESH = pl.DeviceIdType.MESH
F32 = jnp.float32
BF16 = jnp.bfloat16


def kernel_table(kept_freqs, sample_index):
    phase_index = kept_freqs[:, None] * sample_index[None, :] % NFFT
    angle_val = 2.0 * math.pi / NFFT * phase_index.astype(F32)
    window = 0.5 - 0.5 * jnp.cos(2.0 * math.pi / NFFT * sample_index.astype(F32))
    norm_scale = 2.0 / math.sqrt(NFFT)
    real_rows = window[None, :] * jnp.cos(angle_val) * norm_scale
    imag_rows = -window[None, :] * jnp.sin(angle_val) * norm_scale
    return jnp.concatenate([real_rows, imag_rows], axis=0)


def round_up(value, step):
    return (value + step - 1) // step * step


def half_mask(nf, lanes):
    lane = lax.broadcasted_iota(jnp.int32, (8, lanes), 1)
    return lane % (2 * nf) < nf


def swap_halves(r, nf):
    lanes = r.shape[1]
    left = pltpu.roll(r, lanes - nf, 1)
    right = pltpu.roll(r, nf, 1)
    return jnp.where(half_mask(nf, lanes), left, right)


def diagonal(nf, lanes):
    row = lax.broadcasted_iota(jnp.int32, (nf, lanes), 0)
    lane = lax.broadcasted_iota(jnp.int32, (nf, lanes), 1)
    return lane % nf == row


def exchange_kernel(dims, x_ref, starts_ref, table_ref, spec_ref, cross_ref,
                    arrived, w_ref, spec, gram, rows_a, rows_b, slots_ta, slots_ga,
                    send_sem, recv_sem, own_sem, out_sem, sa_sem, ra_sem, sb_sem, rb_sem):
    n, nz, nb, nf, pts, chunks = dims
    me = lax.axis_index("ta")
    mz = lax.axis_index("ga")
    times = x_ref.shape[0]
    rows = nb * 2 * nf
    order = list(range(1, n))

    barrier = pltpu.get_barrier_semaphore()
    for o in order:
        pl.semaphore_signal(barrier, inc=1, device_id=(lax.rem(me + o, n), mz), device_id_type=MESH)
    for o in range(1, nz):
        pl.semaphore_signal(barrier, inc=1, device_id=(me, lax.rem(mz + o, nz)), device_id_type=MESH)
    pl.semaphore_wait(barrier, n - 1 + nz - 1)

    def piece(k, o):
        c0, cw = chunks[k]
        peer = lax.rem(me + o, n)
        src_col = pl.multiple_of(peer * pts + c0, 128)
        dst_row = pl.multiple_of(me * times, times)
        return pltpu.make_async_remote_copy(
            src_ref=x_ref.at[:, pl.ds(src_col, cw)],
            dst_ref=arrived.at[pl.ds(dst_row, times), pl.ds(c0, cw)],
            send_sem=send_sem.at[k, o],
            recv_sem=recv_sem.at[k, o],
            device_id=(peer, mz),
            device_id_type=MESH,
        )

    def own(k):
        c0, cw = chunks[k]
        src_col = pl.multiple_of(me * pts + c0, 128)
        dst_row = pl.multiple_of(me * times, times)
        return pltpu.make_async_copy(
            x_ref.at[:, pl.ds(src_col, cw)],
            arrived.at[pl.ds(dst_row, times), pl.ds(c0, cw)],
            own_sem.at[k],
        )

    for k in range(len(chunks)):
        for o in order:
            piece(k, o).start()
        own(k).start()

    total_times = n * times
    lag = (lax.broadcasted_iota(jnp.int32, (NFFT, total_times), 1)
           - lax.broadcasted_iota(jnp.int32, (NFFT, total_times), 0))

    def build(b, carry):
        shift = jnp.where(lag == starts_ref[b], 1.0, 0.0).astype(BF16)
        placed = jnp.dot(table_ref[...], shift, preferred_element_type=F32)
        w_ref[pl.ds(pl.multiple_of(b * 2 * nf, 2 * nf), 2 * nf), :] = placed.astype(BF16)
        return carry

    lax.fori_loop(0, nb, build, 0)
    gram[...] = jnp.zeros_like(gram)
    rows_a[...] = jnp.zeros_like(rows_a)
    rows_b[...] = jnp.zeros_like(rows_b)

    def out_copy(k):
        c0, cw = chunks[k]
        return pltpu.make_async_copy(
            spec.at[:, pl.ds(c0, cw)], spec_ref.at[:, pl.ds(c0, cw)], out_sem.at[k])

    for k, (c0, cw) in enumerate(chunks):
        own(k).wait()
        for o in order:
            piece(k, o).wait_recv()
        s = jnp.dot(w_ref[...], arrived[:, c0:c0 + cw], preferred_element_type=F32).astype(BF16)
        spec[:, c0:c0 + cw] = s
        out_copy(k).start()
        gram[:, :rows] += lax.dot_general(
            s, s, (((1,), (1,)), ((), ())), preferred_element_type=F32)

    lanes = gram.shape[1]
    keep = diagonal(nf, lanes)
    for b in range(nb):
        top = gram[2 * b * nf:(2 * b + 1) * nf, :]
        low = gram[(2 * b + 1) * nf:(2 * b + 2) * nf, :]
        rows_a[b:b + 1, :] = jnp.sum(jnp.where(keep, top, 0.0), axis=0, keepdims=True)
        rows_b[b:b + 1, :] = jnp.sum(jnp.where(keep, low, 0.0), axis=0, keepdims=True)
    swapped = swap_halves(rows_b[...], nf)
    local = rows_a[...] + jnp.where(half_mask(nf, lanes), swapped, -swapped)

    slots_ta[me] = local

    def stage_a(o):
        peer = lax.rem(me + o, n)
        return pltpu.make_async_remote_copy(
            src_ref=slots_ta.at[me], dst_ref=slots_ta.at[me],
            send_sem=sa_sem.at[o], recv_sem=ra_sem.at[o],
            device_id=(peer, mz), device_id_type=MESH)

    def stage_b(o):
        peer = lax.rem(mz + o, nz)
        return pltpu.make_async_remote_copy(
            src_ref=slots_ga.at[mz], dst_ref=slots_ga.at[mz],
            send_sem=sb_sem.at[o], recv_sem=rb_sem.at[o],
            device_id=(me, peer), device_id_type=MESH)

    for o in order:
        stage_a(o).start()
    for o in order:
        stage_a(o).wait_recv()
    plane = slots_ta[0]
    for i in range(1, n):
        plane = plane + slots_ta[i]
    slots_ga[mz] = plane
    for o in range(1, nz):
        stage_b(o).start()
    for o in range(1, nz):
        stage_b(o).wait_recv()
    whole = slots_ga[0]
    for i in range(1, nz):
        whole = whole + slots_ga[i]
    cross_ref[...] = whole

    for k in range(len(chunks)):
        out_copy(k).wait()
        for o in order:
            piece(k, o).wait_send()
    for o in order:
        stage_a(o).wait_send()
    for o in range(1, nz):
        stage_b(o).wait_send()


def power_kernel(dims, scale, cross_ref, spec_ref, spec_out, power_out, high, low):
    nb, nf = dims
    rows = nb * 2 * nf
    lanes = cross_ref.shape[1]

    @pl.when(pl.program_id(0) == 0)
    def _():
        cross = cross_ref[...] * scale
        swapped = swap_halves(cross, nf)
        turned = jnp.where(half_mask(nf, lanes), -swapped, swapped)
        keep = diagonal(nf, lanes)
        for b in range(nb):
            for c, source in enumerate((cross, turned)):
                m = jnp.where(keep, jnp.broadcast_to(source[b:b + 1, :], (nf, lanes)), 0.0)[:, :rows]
                hi = m.astype(BF16)
                r0 = (2 * b + c) * nf
                high[r0:r0 + nf, :] = hi
                low[r0:r0 + nf, :] = (m - hi.astype(F32)).astype(BF16)

    s = spec_ref[...]
    spec_out[...] = s
    power_out[...] = (jnp.dot(high[...], s, preferred_element_type=F32)
                      + jnp.dot(low[...], s, preferred_element_type=F32))


def shards(snapshots, block_starts, kept_freqs):
    n = lax.axis_size("ta")
    nz = lax.axis_size("ga")
    nb = block_starts.shape[0]
    nf = kept_freqs.shape[0]
    times = snapshots.shape[0]
    pts = snapshots.shape[2] // n
    rows = nb * 2 * nf
    lanes = round_up(rows, 128)
    assert nb <= 8
    width = pts // 4
    chunks = [(c0, width) for c0 in range(0, pts, width)]
    nk = len(chunks)
    table = kernel_table(kept_freqs, jnp.arange(NFFT, dtype=jnp.int32)).astype(BF16)
    x = snapshots.reshape(times, snapshots.shape[2])
    dma = pltpu.SemaphoreType.DMA
    spectra, cross = pl.pallas_call(
        functools.partial(exchange_kernel, (n, nz, nb, nf, pts, chunks)),
        out_shape=(jax.ShapeDtypeStruct((rows, pts), BF16),
                   jax.ShapeDtypeStruct((8, lanes), F32)),
        in_specs=[pl.BlockSpec(memory_space=pltpu.HBM),
                  pl.BlockSpec(memory_space=pltpu.SMEM),
                  pl.BlockSpec(memory_space=pltpu.VMEM)],
        out_specs=(pl.BlockSpec(memory_space=pl.ANY), pl.BlockSpec(memory_space=pltpu.VMEM)),
        scratch_shapes=[
            pltpu.VMEM((n * times, pts), BF16),
            pltpu.VMEM((rows, n * times), BF16),
            pltpu.VMEM((rows, pts), BF16),
            pltpu.VMEM((rows, lanes), F32),
            pltpu.VMEM((8, lanes), F32),
            pltpu.VMEM((8, lanes), F32),
            pltpu.VMEM((n, 8, lanes), F32),
            pltpu.VMEM((nz, 8, lanes), F32),
            dma((nk, n)), dma((nk, n)), dma((nk,)), dma((nk,)),
            dma((n,)), dma((n,)), dma((nz,)), dma((nz,)),
        ],
        compiler_params=pltpu.CompilerParams(
            collective_id=0, has_side_effects=True, vmem_limit_bytes=40 * 1024 * 1024),
        name="exchange",
    )(x, block_starts, table)

    tile = pts // 4
    spectra, power = pl.pallas_call(
        functools.partial(power_kernel, (nb, nf), 1.0 / float(nb * pts * n * nz)),
        grid=(pts // tile,),
        out_shape=(jax.ShapeDtypeStruct((rows, pts), BF16),
                   jax.ShapeDtypeStruct((rows, pts), F32)),
        in_specs=[pl.BlockSpec((8, lanes), lambda i: (0, 0)),
                  pl.BlockSpec((rows, tile), lambda i: (0, i))],
        out_specs=(pl.BlockSpec((rows, tile), lambda i: (0, i)),
                   pl.BlockSpec((rows, tile), lambda i: (0, i))),
        scratch_shapes=[pltpu.VMEM((rows, rows), BF16), pltpu.VMEM((rows, rows), BF16)],
        compiler_params=pltpu.CompilerParams(vmem_limit_bytes=32 * 1024 * 1024),
        name="power",
    )(cross, spectra)
    return (spectra.reshape(1, nb, 2, nf, pts), power.reshape(1, nb, 2, nf, pts))


def solution(mesh):
    in_specs = (P("ta", "ga", None), P(), P())
    out_specs = (P("ga", None, None, None, "ta"), P("ga", None, None, None, "ta"))
    return jax.shard_map(shards, mesh=mesh, in_specs=in_specs, out_specs=out_specs, check_vma=False)
```

```python
import functools
import math

import jax
import jax.numpy as jnp
from jax import lax
from jax.experimental import pallas as pl
from jax.experimental.pallas import tpu as pltpu
from jax.sharding import PartitionSpec as P

NFFT = 256
MESH = pl.DeviceIdType.MESH
F32 = jnp.float32
BF16 = jnp.bfloat16


def build_table(phase, freqs, table):
    nf, nfft = phase.shape
    sample = lax.broadcasted_iota(jnp.int32, (1, nfft), 1)

    def phase_row(j, carry):
        phase[pl.ds(j, 1), :] = (freqs[j] * sample) % nfft
        return carry

    lax.fori_loop(0, nf, phase_row, 0)
    angle_val = 2.0 * math.pi / nfft * phase[...].astype(F32)
    window = 0.5 - 0.5 * jnp.cos(2.0 * math.pi / nfft * sample.astype(F32))
    norm_scale = 2.0 / math.sqrt(nfft)
    table[:nf, :] = (window * jnp.cos(angle_val) * norm_scale).astype(BF16)
    table[nf:, :] = (-window * jnp.sin(angle_val) * norm_scale).astype(BF16)


def round_up(value, step):
    return (value + step - 1) // step * step


def half_mask(nf, lanes):
    lane = lax.broadcasted_iota(jnp.int32, (8, lanes), 1)
    return lane % (2 * nf) < nf


def swap_halves(r, nf):
    lanes = r.shape[1]
    left = pltpu.roll(r, lanes - nf, 1)
    right = pltpu.roll(r, nf, 1)
    return jnp.where(half_mask(nf, lanes), left, right)


def diagonal(nf, lanes):
    row = lax.broadcasted_iota(jnp.int32, (nf, lanes), 0)
    lane = lax.broadcasted_iota(jnp.int32, (nf, lanes), 1)
    return lane % nf == row


def exchange_kernel(dims, x_ref, starts_hbm, freqs_hbm, spec_ref, cross_ref,
                    starts_ref, freqs_ref, small_sem, phase, table_ref, arrived, w_ref, spec, gram, rows_a, rows_b, slots_ta, slots_ga,
                    send_sem, recv_sem, own_sem, out_sem, sa_sem, ra_sem, sb_sem, rb_sem):
    n, nz, nb, nf, pts, chunks = dims
    me = lax.axis_index("ta")
    mz = lax.axis_index("ga")
    times = x_ref.shape[0]
    rows = nb * 2 * nf
    order = list(range(1, n))

    barrier = pltpu.get_barrier_semaphore()
    for o in order:
        pl.semaphore_signal(barrier, inc=1, device_id=(lax.rem(me + o, n), mz), device_id_type=MESH)
    for o in range(1, nz):
        pl.semaphore_signal(barrier, inc=1, device_id=(me, lax.rem(mz + o, nz)), device_id_type=MESH)
    pl.semaphore_wait(barrier, n - 1 + nz - 1)

    def piece(k, o):
        c0, cw = chunks[k]
        peer = lax.rem(me + o, n)
        src_col = pl.multiple_of(peer * pts + c0, 128)
        dst_row = pl.multiple_of(me * times, times)
        return pltpu.make_async_remote_copy(
            src_ref=x_ref.at[:, pl.ds(src_col, cw)],
            dst_ref=arrived.at[pl.ds(dst_row, times), pl.ds(c0, cw)],
            send_sem=send_sem.at[k, o],
            recv_sem=recv_sem.at[k, o],
            device_id=(peer, mz),
            device_id_type=MESH,
        )

    def own(k):
        c0, cw = chunks[k]
        src_col = pl.multiple_of(me * pts + c0, 128)
        dst_row = pl.multiple_of(me * times, times)
        return pltpu.make_async_copy(
            x_ref.at[:, pl.ds(src_col, cw)],
            arrived.at[pl.ds(dst_row, times), pl.ds(c0, cw)],
            own_sem.at[k],
        )

    for k in range(len(chunks)):
        for o in order:
            piece(k, o).start()
        own(k).start()

    fetch_starts = pltpu.make_async_copy(starts_hbm, starts_ref, small_sem.at[0])
    fetch_freqs = pltpu.make_async_copy(freqs_hbm, freqs_ref, small_sem.at[1])
    fetch_starts.start()
    fetch_freqs.start()
    fetch_starts.wait()
    fetch_freqs.wait()
    build_table(phase, freqs_ref, table_ref)

    total_times = n * times
    lag = (lax.broadcasted_iota(jnp.int32, (NFFT, total_times), 1)
           - lax.broadcasted_iota(jnp.int32, (NFFT, total_times), 0))

    def build(b, carry):
        shift = jnp.where(lag == starts_ref[b], 1.0, 0.0).astype(BF16)
        placed = jnp.dot(table_ref[...], shift, preferred_element_type=F32)
        w_ref[pl.ds(pl.multiple_of(b * 2 * nf, 2 * nf), 2 * nf), :] = placed.astype(BF16)
        return carry

    lax.fori_loop(0, nb, build, 0)
    gram[...] = jnp.zeros_like(gram)
    rows_a[...] = jnp.zeros_like(rows_a)
    rows_b[...] = jnp.zeros_like(rows_b)

    def out_copy(k):
        c0, cw = chunks[k]
        return pltpu.make_async_copy(
            spec.at[:, pl.ds(c0, cw)], spec_ref.at[:, pl.ds(c0, cw)], out_sem.at[k])

    for k, (c0, cw) in enumerate(chunks):
        own(k).wait()
        for o in order:
            piece(k, o).wait_recv()
        s = jnp.dot(w_ref[...], arrived[:, c0:c0 + cw], preferred_element_type=F32).astype(BF16)
        spec[:, c0:c0 + cw] = s
        out_copy(k).start()
        gram[:, :rows] += lax.dot_general(
            s, s, (((1,), (1,)), ((), ())), preferred_element_type=F32)

    lanes = gram.shape[1]
    keep = diagonal(nf, lanes)
    for b in range(nb):
        top = gram[2 * b * nf:(2 * b + 1) * nf, :]
        low = gram[(2 * b + 1) * nf:(2 * b + 2) * nf, :]
        rows_a[b:b + 1, :] = jnp.sum(jnp.where(keep, top, 0.0), axis=0, keepdims=True)
        rows_b[b:b + 1, :] = jnp.sum(jnp.where(keep, low, 0.0), axis=0, keepdims=True)
    swapped = swap_halves(rows_b[...], nf)
    local = rows_a[...] + jnp.where(half_mask(nf, lanes), swapped, -swapped)

    slots_ta[me] = local

    def stage_a(o):
        peer = lax.rem(me + o, n)
        return pltpu.make_async_remote_copy(
            src_ref=slots_ta.at[me], dst_ref=slots_ta.at[me],
            send_sem=sa_sem.at[o], recv_sem=ra_sem.at[o],
            device_id=(peer, mz), device_id_type=MESH)

    def stage_b(o):
        peer = lax.rem(mz + o, nz)
        return pltpu.make_async_remote_copy(
            src_ref=slots_ga.at[mz], dst_ref=slots_ga.at[mz],
            send_sem=sb_sem.at[o], recv_sem=rb_sem.at[o],
            device_id=(me, peer), device_id_type=MESH)

    for o in order:
        stage_a(o).start()
    for o in order:
        stage_a(o).wait_recv()
    plane = slots_ta[0]
    for i in range(1, n):
        plane = plane + slots_ta[i]
    slots_ga[mz] = plane
    for o in range(1, nz):
        stage_b(o).start()
    for o in range(1, nz):
        stage_b(o).wait_recv()
    whole = slots_ga[0]
    for i in range(1, nz):
        whole = whole + slots_ga[i]
    cross_ref[...] = whole

    for k in range(len(chunks)):
        out_copy(k).wait()
        for o in order:
            piece(k, o).wait_send()
    for o in order:
        stage_a(o).wait_send()
    for o in range(1, nz):
        stage_b(o).wait_send()


def power_kernel(dims, scale, cross_ref, spec_ref, spec_out, power_out, mix):
    nb, nf = dims
    rows = nb * 2 * nf
    lanes = cross_ref.shape[1]

    @pl.when(pl.program_id(0) == 0)
    def _():
        cross = cross_ref[...] * scale
        swapped = swap_halves(cross, nf)
        turned = jnp.where(half_mask(nf, lanes), -swapped, swapped)
        keep = diagonal(nf, lanes)
        for b in range(nb):
            for c, source in enumerate((cross, turned)):
                m = jnp.where(keep, jnp.broadcast_to(source[b:b + 1, :], (nf, lanes)), 0.0)[:, :rows]
                r0 = (2 * b + c) * nf
                mix[r0:r0 + nf, :] = m.astype(BF16)

    s = spec_ref[...]
    spec_out[...] = s
    power_out[...] = jnp.dot(mix[...], s, preferred_element_type=F32)


def shards(snapshots, block_starts, kept_freqs):
    n = lax.axis_size("ta")
    nz = lax.axis_size("ga")
    nb = block_starts.shape[0]
    nf = kept_freqs.shape[0]
    times = snapshots.shape[0]
    pts = snapshots.shape[2] // n
    rows = nb * 2 * nf
    lanes = round_up(rows, 128)
    assert nb <= 8
    width = pts // 4
    chunks = [(c0, width) for c0 in range(0, pts, width)]
    nk = len(chunks)
    operands = [pltpu.with_memory_space_constraint(a, pltpu.HBM) for a in (
        snapshots.reshape(times, snapshots.shape[2]), block_starts, kept_freqs)]
    dma = pltpu.SemaphoreType.DMA
    spectra, cross = pl.pallas_call(
        functools.partial(exchange_kernel, (n, nz, nb, nf, pts, chunks)),
        out_shape=(jax.ShapeDtypeStruct((rows, pts), BF16),
                   jax.ShapeDtypeStruct((8, lanes), F32)),
        in_specs=[pl.BlockSpec(memory_space=pl.ANY)] * 3,
        out_specs=(pl.BlockSpec(memory_space=pl.ANY), pl.BlockSpec(memory_space=pltpu.VMEM)),
        scratch_shapes=[
            pltpu.SMEM((nb,), jnp.int32),
            pltpu.SMEM((nf,), jnp.int32),
            dma((2,)),
            pltpu.VMEM((nf, NFFT), jnp.int32),
            pltpu.VMEM((2 * nf, NFFT), BF16),
            pltpu.VMEM((n * times, pts), BF16),
            pltpu.VMEM((rows, n * times), BF16),
            pltpu.VMEM((rows, pts), BF16),
            pltpu.VMEM((rows, lanes), F32),
            pltpu.VMEM((8, lanes), F32),
            pltpu.VMEM((8, lanes), F32),
            pltpu.VMEM((n, 8, lanes), F32),
            pltpu.VMEM((nz, 8, lanes), F32),
            dma((nk, n)), dma((nk, n)), dma((nk,)), dma((nk,)),
            dma((n,)), dma((n,)), dma((nz,)), dma((nz,)),
        ],
        compiler_params=pltpu.CompilerParams(
            collective_id=0, has_side_effects=True, vmem_limit_bytes=40 * 1024 * 1024),
        name="exchange",
    )(*operands)

    tile = pts // 4
    spectra, power = pl.pallas_call(
        functools.partial(power_kernel, (nb, nf), 1.0 / float(nb * pts * n * nz)),
        grid=(pts // tile,),
        out_shape=(jax.ShapeDtypeStruct((rows, pts), BF16),
                   jax.ShapeDtypeStruct((rows, pts), F32)),
        in_specs=[pl.BlockSpec((8, lanes), lambda i: (0, 0)),
                  pl.BlockSpec((rows, tile), lambda i: (0, i))],
        out_specs=(pl.BlockSpec((rows, tile), lambda i: (0, i)),
                   pl.BlockSpec((rows, tile), lambda i: (0, i))),
        scratch_shapes=[pltpu.VMEM((rows, rows), BF16)],
        compiler_params=pltpu.CompilerParams(vmem_limit_bytes=32 * 1024 * 1024),
        name="power",
    )(cross, spectra)
    return (spectra.reshape(1, nb, 2, nf, pts), power.reshape(1, nb, 2, nf, pts))


def solution(mesh):
    in_specs = (P("ta", "ga", None), P(), P())
    out_specs = (P("ga", None, None, None, "ta"), P("ga", None, None, None, "ta"))
    return jax.shard_map(shards, mesh=mesh, in_specs=in_specs, out_specs=out_specs, check_vma=False)
```

```python
import functools
import math

import jax
import jax.numpy as jnp
from jax import lax
from jax.experimental import pallas as pl
from jax.experimental.pallas import tpu as pltpu
from jax.sharding import PartitionSpec as P

NFFT = 256
MESH = pl.DeviceIdType.MESH
F32 = jnp.float32
BF16 = jnp.bfloat16


def build_table(phase, freqs, table):
    nf, nfft = phase.shape
    sample = lax.broadcasted_iota(jnp.int32, (1, nfft), 1)

    def phase_row(j, carry):
        phase[pl.ds(j, 1), :] = (freqs[j] * sample) % nfft
        return carry

    lax.fori_loop(0, nf, phase_row, 0)
    angle_val = 2.0 * math.pi / nfft * phase[...].astype(F32)
    window = 0.5 - 0.5 * jnp.cos(2.0 * math.pi / nfft * sample.astype(F32))
    norm_scale = 2.0 / math.sqrt(nfft)
    table[:nf, :] = (window * jnp.cos(angle_val) * norm_scale).astype(BF16)
    table[nf:, :] = (-window * jnp.sin(angle_val) * norm_scale).astype(BF16)


def round_up(value, step):
    return (value + step - 1) // step * step


def half_mask(nf, lanes):
    lane = lax.broadcasted_iota(jnp.int32, (8, lanes), 1)
    return lane % (2 * nf) < nf


def swap_halves(r, nf):
    lanes = r.shape[1]
    left = pltpu.roll(r, lanes - nf, 1)
    right = pltpu.roll(r, nf, 1)
    return jnp.where(half_mask(nf, lanes), left, right)


def diagonal(nf, lanes):
    row = lax.broadcasted_iota(jnp.int32, (nf, lanes), 0)
    lane = lax.broadcasted_iota(jnp.int32, (nf, lanes), 1)
    return lane % nf == row


def direct_plan(n, pts, chunks, x_ref, arrived, send_sem, recv_sem):
    me = lax.axis_index("ta")
    mz = lax.axis_index("ga")
    times = x_ref.shape[0]
    every = [(k, o) for k in range(len(chunks)) for o in range(1, n)]

    def piece(k, o):
        c0, cw = chunks[k]
        peer = lax.rem(me + o, n)
        return pltpu.make_async_remote_copy(
            src_ref=x_ref.at[:, pl.ds(pl.multiple_of(peer * pts + c0, 128), cw)],
            dst_ref=arrived.at[pl.ds(pl.multiple_of(me * times, times), times), pl.ds(c0, cw)],
            send_sem=send_sem.at[k, o],
            recv_sem=recv_sem.at[k, o],
            device_id=(peer, mz),
            device_id_type=MESH,
        )

    def begin():
        for k, o in every:
            piece(k, o).start()

    def follow():
        pass

    def receive(k):
        for o in range(1, n):
            piece(k, o).wait_recv()

    def finish():
        for k, o in every:
            piece(k, o).wait_send()

    return begin, follow, receive, finish


def square_plan(pts, chunks, x_ref, arrived, relay, send_sem, recv_sem):
    me = lax.axis_index("ta")
    mz = lax.axis_index("ga")
    times = x_ref.shape[0]
    core, x, y = me % 2, (me // 2) % 2, me // 4
    count = range(len(chunks))

    def index(yy, xx, cc):
        return (yy * 2 + xx) * 2 + cc

    def copy(k, src, dst, slot_out, slot_in, device):
        return pltpu.make_async_remote_copy(
            src_ref=src, dst_ref=dst, send_sem=send_sem.at[k, slot_out], recv_sem=recv_sem.at[k, slot_in],
            device_id=(device, mz), device_id_type=MESH)

    def columns(k, owner):
        c0, cw = chunks[k]
        return x_ref.at[:, pl.ds(pl.multiple_of(owner * pts + c0, 128), cw)]

    def place(k, source):
        c0, cw = chunks[k]
        return arrived.at[pl.ds(pl.multiple_of(source * times, times), times), pl.ds(c0, cw)]

    def to_relay(k, c):
        c0, cw = chunks[k]
        return copy(k, columns(k, index(1 - y, 1 - x, c)), relay.at[c, :, pl.ds(c0, cw)],
                    c, c, index(y, 1 - x, core))

    def along_x(k, c):
        peer = index(y, 1 - x, c)
        return copy(k, columns(k, peer), place(k, me), 2 + c, 2 + core, peer)

    def along_y(k, c):
        peer = index(1 - y, x, c)
        return copy(k, columns(k, peer), place(k, me), 4 + c, 4 + core, peer)

    def onward(k, c):
        c0, cw = chunks[k]
        return copy(k, relay.at[c, :, pl.ds(c0, cw)], place(k, index(y, 1 - x, core)),
                    7 + c, 7 + core, index(1 - y, x, c))

    def across(k):
        peer = index(y, x, 1 - core)
        return copy(k, columns(k, peer), place(k, me), 6, 6, peer)

    def arrival(k, slot):
        return copy(k, place(k, me), place(k, me), slot, slot, me)

    def begin():
        for k in count:
            for c in range(2):
                to_relay(k, c).start()
                along_y(k, c).start()
        for k in count:
            across(k).start()

    def follow():
        for k in count:
            for c in range(2):
                to_relay(k, c).wait_recv()
                onward(k, c).start()
            for c in range(2):
                along_x(k, c).start()

    def receive(k):
        across(k).wait_recv()
        for slot in (2, 3, 4, 5, 7, 8):
            arrival(k, slot).wait_recv()

    def finish():
        for k in count:
            for c in range(2):
                to_relay(k, c).wait_send()
                along_x(k, c).wait_send()
                along_y(k, c).wait_send()
                onward(k, c).wait_send()
            across(k).wait_send()

    return begin, follow, receive, finish


def exchange_kernel(dims, x_ref, starts_hbm, freqs_hbm, spec_ref, cross_ref,
                    starts_ref, freqs_ref, small_sem, phase, table_ref, arrived, w_ref, spec, gram, rows_a, rows_b, slots_ta, slots_ga,
                    send_sem, recv_sem, own_sem, out_sem, sa_sem, ra_sem, sb_sem, rb_sem, relay=None):
    n, nz, nb, nf, pts, chunks = dims
    me = lax.axis_index("ta")
    mz = lax.axis_index("ga")
    times = x_ref.shape[0]
    rows = nb * 2 * nf
    order = list(range(1, n))

    barrier = pltpu.get_barrier_semaphore()
    for o in order:
        pl.semaphore_signal(barrier, inc=1, device_id=(lax.rem(me + o, n), mz), device_id_type=MESH)
    for o in range(1, nz):
        pl.semaphore_signal(barrier, inc=1, device_id=(me, lax.rem(mz + o, nz)), device_id_type=MESH)
    pl.semaphore_wait(barrier, n - 1 + nz - 1)

    if relay is None:
        plan = direct_plan(n, pts, chunks, x_ref, arrived, send_sem, recv_sem)
    else:
        plan = square_plan(pts, chunks, x_ref, arrived, relay, send_sem, recv_sem)
    begin, follow, receive, finish = plan

    def own(k):
        c0, cw = chunks[k]
        src_col = pl.multiple_of(me * pts + c0, 128)
        dst_row = pl.multiple_of(me * times, times)
        return pltpu.make_async_copy(
            x_ref.at[:, pl.ds(src_col, cw)],
            arrived.at[pl.ds(dst_row, times), pl.ds(c0, cw)],
            own_sem.at[k],
        )

    begin()
    for k in range(len(chunks)):
        own(k).start()

    fetch_starts = pltpu.make_async_copy(starts_hbm, starts_ref, small_sem.at[0])
    fetch_freqs = pltpu.make_async_copy(freqs_hbm, freqs_ref, small_sem.at[1])
    fetch_starts.start()
    fetch_freqs.start()
    fetch_starts.wait()
    fetch_freqs.wait()
    build_table(phase, freqs_ref, table_ref)

    total_times = n * times
    lag = (lax.broadcasted_iota(jnp.int32, (NFFT, total_times), 1)
           - lax.broadcasted_iota(jnp.int32, (NFFT, total_times), 0))

    def build(b, carry):
        shift = jnp.where(lag == starts_ref[b], 1.0, 0.0).astype(BF16)
        placed = jnp.dot(table_ref[...], shift, preferred_element_type=F32)
        w_ref[pl.ds(pl.multiple_of(b * 2 * nf, 2 * nf), 2 * nf), :] = placed.astype(BF16)
        return carry

    lax.fori_loop(0, nb, build, 0)
    gram[...] = jnp.zeros_like(gram)
    rows_a[...] = jnp.zeros_like(rows_a)
    rows_b[...] = jnp.zeros_like(rows_b)

    follow()

    def out_copy(k):
        c0, cw = chunks[k]
        return pltpu.make_async_copy(
            spec.at[:, pl.ds(c0, cw)], spec_ref.at[:, pl.ds(c0, cw)], out_sem.at[k])

    for k, (c0, cw) in enumerate(chunks):
        own(k).wait()
        receive(k)
        s = jnp.dot(w_ref[...], arrived[:, c0:c0 + cw], preferred_element_type=F32).astype(BF16)
        spec[:, c0:c0 + cw] = s
        out_copy(k).start()
        gram[:, :rows] += lax.dot_general(
            s, s, (((1,), (1,)), ((), ())), preferred_element_type=F32)

    lanes = gram.shape[1]
    keep = diagonal(nf, lanes)
    for b in range(nb):
        top = gram[2 * b * nf:(2 * b + 1) * nf, :]
        low = gram[(2 * b + 1) * nf:(2 * b + 2) * nf, :]
        rows_a[b:b + 1, :] = jnp.sum(jnp.where(keep, top, 0.0), axis=0, keepdims=True)
        rows_b[b:b + 1, :] = jnp.sum(jnp.where(keep, low, 0.0), axis=0, keepdims=True)
    swapped = swap_halves(rows_b[...], nf)
    local = rows_a[...] + jnp.where(half_mask(nf, lanes), swapped, -swapped)

    slots_ta[me] = local

    def stage_a(o):
        peer = lax.rem(me + o, n)
        return pltpu.make_async_remote_copy(
            src_ref=slots_ta.at[me], dst_ref=slots_ta.at[me],
            send_sem=sa_sem.at[o], recv_sem=ra_sem.at[o],
            device_id=(peer, mz), device_id_type=MESH)

    def stage_b(o):
        peer = lax.rem(mz + o, nz)
        return pltpu.make_async_remote_copy(
            src_ref=slots_ga.at[mz], dst_ref=slots_ga.at[mz],
            send_sem=sb_sem.at[o], recv_sem=rb_sem.at[o],
            device_id=(me, peer), device_id_type=MESH)

    for o in order:
        stage_a(o).start()
    for o in order:
        stage_a(o).wait_recv()
    plane = slots_ta[0]
    for i in range(1, n):
        plane = plane + slots_ta[i]
    slots_ga[mz] = plane
    for o in range(1, nz):
        stage_b(o).start()
    for o in range(1, nz):
        stage_b(o).wait_recv()
    whole = slots_ga[0]
    for i in range(1, nz):
        whole = whole + slots_ga[i]
    cross_ref[...] = whole

    for k in range(len(chunks)):
        out_copy(k).wait()
    finish()
    for o in order:
        stage_a(o).wait_send()
    for o in range(1, nz):
        stage_b(o).wait_send()


def power_kernel(dims, scale, cross_ref, spec_ref, spec_out, power_out, mix):
    nb, nf = dims
    rows = nb * 2 * nf
    lanes = cross_ref.shape[1]

    @pl.when(pl.program_id(0) == 0)
    def _():
        cross = cross_ref[...] * scale
        swapped = swap_halves(cross, nf)
        turned = jnp.where(half_mask(nf, lanes), -swapped, swapped)
        keep = diagonal(nf, lanes)
        for b in range(nb):
            for c, source in enumerate((cross, turned)):
                m = jnp.where(keep, jnp.broadcast_to(source[b:b + 1, :], (nf, lanes)), 0.0)[:, :rows]
                r0 = (2 * b + c) * nf
                mix[r0:r0 + nf, :] = m.astype(BF16)

    s = spec_ref[...]
    spec_out[...] = s
    power_out[...] = jnp.dot(mix[...], s, preferred_element_type=F32)


def shards(snapshots, block_starts, kept_freqs):
    n = lax.axis_size("ta")
    nz = lax.axis_size("ga")
    nb = block_starts.shape[0]
    nf = kept_freqs.shape[0]
    times = snapshots.shape[0]
    pts = snapshots.shape[2] // n
    rows = nb * 2 * nf
    lanes = round_up(rows, 128)
    assert nb <= 8
    square = n == 8
    width = pts // 8
    chunks = [(0, 2 * width), (2 * width, 2 * width), (4 * width, 2 * width), (6 * width, width), (7 * width, width)]
    nk = len(chunks)
    operands = [pltpu.with_memory_space_constraint(a, pltpu.HBM) for a in (
        snapshots.reshape(times, snapshots.shape[2]), block_starts, kept_freqs)]
    dma = pltpu.SemaphoreType.DMA
    spectra, cross = pl.pallas_call(
        functools.partial(exchange_kernel, (n, nz, nb, nf, pts, chunks)),
        out_shape=(jax.ShapeDtypeStruct((rows, pts), BF16),
                   jax.ShapeDtypeStruct((8, lanes), F32)),
        in_specs=[pl.BlockSpec(memory_space=pl.ANY)] * 3,
        out_specs=(pl.BlockSpec(memory_space=pl.ANY), pl.BlockSpec(memory_space=pltpu.VMEM)),
        scratch_shapes=[
            pltpu.SMEM((nb,), jnp.int32),
            pltpu.SMEM((nf,), jnp.int32),
            dma((2,)),
            pltpu.VMEM((nf, NFFT), jnp.int32),
            pltpu.VMEM((2 * nf, NFFT), BF16),
            pltpu.VMEM((n * times, pts), BF16),
            pltpu.VMEM((rows, n * times), BF16),
            pltpu.VMEM((rows, pts), BF16),
            pltpu.VMEM((rows, lanes), F32),
            pltpu.VMEM((8, lanes), F32),
            pltpu.VMEM((8, lanes), F32),
            pltpu.VMEM((n, 8, lanes), F32),
            pltpu.VMEM((nz, 8, lanes), F32),
            dma((nk, max(n, 9))), dma((nk, max(n, 9))), dma((nk,)), dma((nk,)),
            dma((n,)), dma((n,)), dma((nz,)), dma((nz,)),
        ] + ([pltpu.VMEM((2, times, pts), BF16)] if square else []),
        compiler_params=pltpu.CompilerParams(
            collective_id=0, has_side_effects=True, vmem_limit_bytes=40 * 1024 * 1024),
        name="exchange",
    )(*operands)

    tile = pts // 4
    spectra, power = pl.pallas_call(
        functools.partial(power_kernel, (nb, nf), 1.0 / float(nb * pts * n * nz)),
        grid=(pts // tile,),
        out_shape=(jax.ShapeDtypeStruct((rows, pts), BF16),
                   jax.ShapeDtypeStruct((rows, pts), F32)),
        in_specs=[pl.BlockSpec((8, lanes), lambda i: (0, 0)),
                  pl.BlockSpec((rows, tile), lambda i: (0, i))],
        out_specs=(pl.BlockSpec((rows, tile), lambda i: (0, i)),
                   pl.BlockSpec((rows, tile), lambda i: (0, i))),
        scratch_shapes=[pltpu.VMEM((rows, rows), BF16)],
        compiler_params=pltpu.CompilerParams(vmem_limit_bytes=32 * 1024 * 1024),
        name="power",
    )(cross, spectra)
    return (spectra.reshape(1, nb, 2, nf, pts), power.reshape(1, nb, 2, nf, pts))


def solution(mesh):
    in_specs = (P("ta", "ga", None), P(), P())
    out_specs = (P("ga", None, None, None, "ta"), P("ga", None, None, None, "ta"))
    return jax.shard_map(shards, mesh=mesh, in_specs=in_specs, out_specs=out_specs, check_vma=False)
```

```python
import functools
import math

import jax
import jax.numpy as jnp
from jax import lax
from jax.experimental import pallas as pl
from jax.experimental.pallas import tpu as pltpu
from jax.sharding import PartitionSpec as P

NFFT = 256
POWER_TILES = 2
MESH = pl.DeviceIdType.MESH
F32 = jnp.float32
BF16 = jnp.bfloat16


def build_table(phase, freqs, table):
    nf, nfft = phase.shape
    sample = lax.broadcasted_iota(jnp.int32, (1, nfft), 1)

    def phase_row(j, carry):
        phase[pl.ds(j, 1), :] = (freqs[j] * sample) % nfft
        return carry

    lax.fori_loop(0, nf, phase_row, 0)
    angle_val = 2.0 * math.pi / nfft * phase[...].astype(F32)
    window = 0.5 - 0.5 * jnp.cos(2.0 * math.pi / nfft * sample.astype(F32))
    norm_scale = 2.0 / math.sqrt(nfft)
    table[:nf, :] = (window * jnp.cos(angle_val) * norm_scale).astype(BF16)
    table[nf:, :] = (-window * jnp.sin(angle_val) * norm_scale).astype(BF16)


def round_up(value, step):
    return (value + step - 1) // step * step


def half_mask(nf, lanes):
    lane = lax.broadcasted_iota(jnp.int32, (8, lanes), 1)
    return lane % (2 * nf) < nf


def swap_halves(r, nf):
    lanes = r.shape[1]
    left = pltpu.roll(r, lanes - nf, 1)
    right = pltpu.roll(r, nf, 1)
    return jnp.where(half_mask(nf, lanes), left, right)


def diagonal(nf, lanes):
    row = lax.broadcasted_iota(jnp.int32, (nf, lanes), 0)
    lane = lax.broadcasted_iota(jnp.int32, (nf, lanes), 1)
    return lane % nf == row


def direct_plan(n, pts, chunks, x_ref, arrived, send_sem, recv_sem):
    me = lax.axis_index("ta")
    mz = lax.axis_index("ga")
    times = x_ref.shape[0]
    every = [(k, o) for k in range(len(chunks)) for o in range(1, n)]

    def piece(k, o):
        c0, cw = chunks[k]
        peer = lax.rem(me + o, n)
        return pltpu.make_async_remote_copy(
            src_ref=x_ref.at[:, pl.ds(pl.multiple_of(peer * pts + c0, 128), cw)],
            dst_ref=arrived.at[pl.ds(pl.multiple_of(me * times, times), times), pl.ds(c0, cw)],
            send_sem=send_sem.at[k, o],
            recv_sem=recv_sem.at[k, o],
            device_id=(peer, mz),
            device_id_type=MESH,
        )

    def begin():
        for k, o in every:
            piece(k, o).start()

    def follow():
        pass

    def receive(k):
        for o in range(1, n):
            piece(k, o).wait_recv()

    def finish():
        for k, o in every:
            piece(k, o).wait_send()

    return begin, follow, receive, finish


def square_plan(pts, chunks, x_ref, arrived, relay, send_sem, recv_sem):
    me = lax.axis_index("ta")
    mz = lax.axis_index("ga")
    times = x_ref.shape[0]
    core, x, y = me % 2, (me // 2) % 2, me // 4
    count = range(len(chunks))

    def index(yy, xx, cc):
        return (yy * 2 + xx) * 2 + cc

    def copy(k, src, dst, slot_out, slot_in, device):
        return pltpu.make_async_remote_copy(
            src_ref=src, dst_ref=dst, send_sem=send_sem.at[k, slot_out], recv_sem=recv_sem.at[k, slot_in],
            device_id=(device, mz), device_id_type=MESH)

    def columns(k, owner):
        c0, cw = chunks[k]
        return x_ref.at[:, pl.ds(pl.multiple_of(owner * pts + c0, 128), cw)]

    def place(k, source):
        c0, cw = chunks[k]
        return arrived.at[pl.ds(pl.multiple_of(source * times, times), times), pl.ds(c0, cw)]

    def to_relay(k, c):
        c0, cw = chunks[k]
        return copy(k, columns(k, index(1 - y, 1 - x, c)), relay.at[c, :, pl.ds(c0, cw)],
                    c, c, index(y, 1 - x, core))

    def along_x(k, c):
        peer = index(y, 1 - x, c)
        return copy(k, columns(k, peer), place(k, me), 2 + c, 2 + core, peer)

    def along_y(k, c):
        peer = index(1 - y, x, c)
        return copy(k, columns(k, peer), place(k, me), 4 + c, 4 + core, peer)

    def onward(k, c):
        c0, cw = chunks[k]
        return copy(k, relay.at[c, :, pl.ds(c0, cw)], place(k, index(y, 1 - x, core)),
                    7 + c, 7 + core, index(1 - y, x, c))

    def across(k):
        peer = index(y, x, 1 - core)
        return copy(k, columns(k, peer), place(k, me), 6, 6, peer)

    def arrival(k, slot):
        return copy(k, place(k, me), place(k, me), slot, slot, me)

    def begin():
        for k in count:
            for c in range(2):
                to_relay(k, c).start()
                along_y(k, c).start()
        for k in count:
            across(k).start()

    def follow():
        for k in count:
            for c in range(2):
                to_relay(k, c).wait_recv()
                onward(k, c).start()
            for c in range(2):
                along_x(k, c).start()

    def receive(k):
        across(k).wait_recv()
        for slot in (2, 3, 4, 5, 7, 8):
            arrival(k, slot).wait_recv()

    def finish():
        for k in count:
            for c in range(2):
                to_relay(k, c).wait_send()
                along_x(k, c).wait_send()
                along_y(k, c).wait_send()
                onward(k, c).wait_send()
            across(k).wait_send()

    return begin, follow, receive, finish


def exchange_kernel(dims, x_ref, starts_hbm, freqs_hbm, spec_ref, cross_ref,
                    starts_ref, freqs_ref, small_sem, phase, table_ref, arrived, w_ref, spec, gram, rows_a, rows_b, slots_ta, slots_ga,
                    send_sem, recv_sem, own_sem, out_sem, sa_sem, ra_sem, sb_sem, rb_sem, relay=None):
    n, nz, nb, nf, pts, chunks = dims
    me = lax.axis_index("ta")
    mz = lax.axis_index("ga")
    times = x_ref.shape[0]
    rows = nb * 2 * nf
    order = list(range(1, n))

    barrier = pltpu.get_barrier_semaphore()
    for o in order:
        pl.semaphore_signal(barrier, inc=1, device_id=(lax.rem(me + o, n), mz), device_id_type=MESH)
    for o in range(1, nz):
        pl.semaphore_signal(barrier, inc=1, device_id=(me, lax.rem(mz + o, nz)), device_id_type=MESH)
    pl.semaphore_wait(barrier, n - 1 + nz - 1)

    if relay is None:
        plan = direct_plan(n, pts, chunks, x_ref, arrived, send_sem, recv_sem)
    else:
        plan = square_plan(pts, chunks, x_ref, arrived, relay, send_sem, recv_sem)
    begin, follow, receive, finish = plan

    def own(k):
        c0, cw = chunks[k]
        src_col = pl.multiple_of(me * pts + c0, 128)
        dst_row = pl.multiple_of(me * times, times)
        return pltpu.make_async_copy(
            x_ref.at[:, pl.ds(src_col, cw)],
            arrived.at[pl.ds(dst_row, times), pl.ds(c0, cw)],
            own_sem.at[k],
        )

    begin()
    for k in range(len(chunks)):
        own(k).start()

    fetch_starts = pltpu.make_async_copy(starts_hbm, starts_ref, small_sem.at[0])
    fetch_freqs = pltpu.make_async_copy(freqs_hbm, freqs_ref, small_sem.at[1])
    fetch_starts.start()
    fetch_freqs.start()
    fetch_starts.wait()
    fetch_freqs.wait()
    build_table(phase, freqs_ref, table_ref)

    total_times = n * times
    lag = (lax.broadcasted_iota(jnp.int32, (NFFT, total_times), 1)
           - lax.broadcasted_iota(jnp.int32, (NFFT, total_times), 0))

    def build(b, carry):
        shift = jnp.where(lag == starts_ref[b], 1.0, 0.0).astype(BF16)
        placed = jnp.dot(table_ref[...], shift, preferred_element_type=F32)
        w_ref[pl.ds(pl.multiple_of(b * 2 * nf, 2 * nf), 2 * nf), :] = placed.astype(BF16)
        return carry

    lax.fori_loop(0, nb, build, 0)
    gram[...] = jnp.zeros_like(gram)
    rows_a[...] = jnp.zeros_like(rows_a)
    rows_b[...] = jnp.zeros_like(rows_b)

    follow()

    def out_copy(k):
        c0, cw = chunks[k]
        return pltpu.make_async_copy(
            spec.at[:, pl.ds(c0, cw)], spec_ref.at[:, pl.ds(c0, cw)], out_sem.at[k])

    for k, (c0, cw) in enumerate(chunks):
        own(k).wait()
        receive(k)
        s = jnp.dot(w_ref[...], arrived[:, c0:c0 + cw], preferred_element_type=F32).astype(BF16)
        spec[:, c0:c0 + cw] = s
        out_copy(k).start()
        gram[:, :rows] += lax.dot_general(
            s, s, (((1,), (1,)), ((), ())), preferred_element_type=F32)

    lanes = gram.shape[1]
    keep = diagonal(nf, lanes)
    for b in range(nb):
        top = gram[2 * b * nf:(2 * b + 1) * nf, :]
        low = gram[(2 * b + 1) * nf:(2 * b + 2) * nf, :]
        rows_a[b:b + 1, :] = jnp.sum(jnp.where(keep, top, 0.0), axis=0, keepdims=True)
        rows_b[b:b + 1, :] = jnp.sum(jnp.where(keep, low, 0.0), axis=0, keepdims=True)
    swapped = swap_halves(rows_b[...], nf)
    local = rows_a[...] + jnp.where(half_mask(nf, lanes), swapped, -swapped)

    slots_ta[me] = local.astype(BF16)

    def stage_a(o):
        peer = lax.rem(me + o, n)
        return pltpu.make_async_remote_copy(
            src_ref=slots_ta.at[me], dst_ref=slots_ta.at[me],
            send_sem=sa_sem.at[o], recv_sem=ra_sem.at[o],
            device_id=(peer, mz), device_id_type=MESH)

    def stage_b(o):
        peer = lax.rem(mz + o, nz)
        return pltpu.make_async_remote_copy(
            src_ref=slots_ga.at[mz], dst_ref=slots_ga.at[mz],
            send_sem=sb_sem.at[o], recv_sem=rb_sem.at[o],
            device_id=(me, peer), device_id_type=MESH)

    for o in order:
        stage_a(o).start()
    for o in order:
        stage_a(o).wait_recv()
    plane = slots_ta[0].astype(F32)
    for i in range(1, n):
        plane = plane + slots_ta[i].astype(F32)
    slots_ga[mz] = plane.astype(BF16)
    for o in range(1, nz):
        stage_b(o).start()
    for o in range(1, nz):
        stage_b(o).wait_recv()
    whole = slots_ga[0].astype(F32)
    for i in range(1, nz):
        whole = whole + slots_ga[i].astype(F32)
    cross_ref[...] = whole

    for k in range(len(chunks)):
        out_copy(k).wait()
    finish()
    for o in order:
        stage_a(o).wait_send()
    for o in range(1, nz):
        stage_b(o).wait_send()


def power_kernel(dims, scale, cross_ref, spec_ref, spec_out, power_out, mix, result, spec_sem, tile_sem):
    nb, nf, tile = dims
    rows, pts = spec_ref.shape
    lanes = cross_ref.shape[1]
    spectra_copy = pltpu.make_async_copy(spec_ref, spec_out, spec_sem)
    spectra_copy.start()
    cross = cross_ref[...] * scale
    swapped = swap_halves(cross, nf)
    turned = jnp.where(half_mask(nf, lanes), -swapped, swapped)
    keep = diagonal(nf, lanes)
    for b in range(nb):
        for c, source in enumerate((cross, turned)):
            m = jnp.where(keep, jnp.broadcast_to(source[b:b + 1, :], (nf, lanes)), 0.0)[:, :rows]
            r0 = (2 * b + c) * nf
            mix[r0:r0 + nf, :] = m.astype(BF16)

    def tile_copy(i):
        part = pl.ds(i * tile, tile)
        return pltpu.make_async_copy(result.at[:, part], power_out.at[:, part], tile_sem.at[i])

    for i in range(pts // tile):
        result[:, i * tile:(i + 1) * tile] = jnp.dot(
            mix[...], spec_ref[:, i * tile:(i + 1) * tile], preferred_element_type=F32)
        tile_copy(i).start()
    for i in range(pts // tile):
        tile_copy(i).wait()
    spectra_copy.wait()


def shards(snapshots, block_starts, kept_freqs):
    n = lax.axis_size("ta")
    nz = lax.axis_size("ga")
    nb = block_starts.shape[0]
    nf = kept_freqs.shape[0]
    times = snapshots.shape[0]
    pts = snapshots.shape[2] // n
    rows = nb * 2 * nf
    lanes = round_up(rows, 128)
    assert nb <= 8
    square = n == 8
    width = pts // 8
    chunks = [(0, 2 * width), (2 * width, 2 * width), (4 * width, 2 * width), (6 * width, width), (7 * width, width)]
    nk = len(chunks)
    operands = [pltpu.with_memory_space_constraint(a, pltpu.HBM) for a in (
        snapshots.reshape(times, snapshots.shape[2]), block_starts, kept_freqs)]
    dma = pltpu.SemaphoreType.DMA
    spectra, cross = pl.pallas_call(
        functools.partial(exchange_kernel, (n, nz, nb, nf, pts, chunks)),
        out_shape=(jax.ShapeDtypeStruct((rows, pts), BF16),
                   jax.ShapeDtypeStruct((8, lanes), F32)),
        in_specs=[pl.BlockSpec(memory_space=pl.ANY)] * 3,
        out_specs=(pl.BlockSpec(memory_space=pl.ANY), pl.BlockSpec(memory_space=pltpu.VMEM)),
        scratch_shapes=[
            pltpu.SMEM((nb,), jnp.int32),
            pltpu.SMEM((nf,), jnp.int32),
            dma((2,)),
            pltpu.VMEM((nf, NFFT), jnp.int32),
            pltpu.VMEM((2 * nf, NFFT), BF16),
            pltpu.VMEM((n * times, pts), BF16),
            pltpu.VMEM((rows, n * times), BF16),
            pltpu.VMEM((rows, pts), BF16),
            pltpu.VMEM((rows, lanes), F32),
            pltpu.VMEM((8, lanes), F32),
            pltpu.VMEM((8, lanes), F32),
            pltpu.VMEM((n, 8, lanes), BF16),
            pltpu.VMEM((nz, 8, lanes), BF16),
            dma((nk, max(n, 9))), dma((nk, max(n, 9))), dma((nk,)), dma((nk,)),
            dma((n,)), dma((n,)), dma((nz,)), dma((nz,)),
        ] + ([pltpu.VMEM((2, times, pts), BF16)] if square else []),
        compiler_params=pltpu.CompilerParams(
            collective_id=0, has_side_effects=True, vmem_limit_bytes=40 * 1024 * 1024),
        name="exchange",
    )(*operands)

    tile = pts // POWER_TILES
    spectra, power = pl.pallas_call(
        functools.partial(power_kernel, (nb, nf, tile), 1.0 / float(nb * pts * n * nz)),
        out_shape=(jax.ShapeDtypeStruct((rows, pts), BF16),
                   jax.ShapeDtypeStruct((rows, pts), F32)),
        in_specs=[pl.BlockSpec(memory_space=pltpu.VMEM)] * 2,
        out_specs=(pl.BlockSpec(memory_space=pltpu.HBM), pl.BlockSpec(memory_space=pltpu.HBM)),
        scratch_shapes=[pltpu.VMEM((rows, rows), BF16), pltpu.VMEM((rows, pts), F32),
                        dma(()), dma((pts // tile,))],
        compiler_params=pltpu.CompilerParams(vmem_limit_bytes=32 * 1024 * 1024),
        name="power",
    )(cross, spectra)
    return (spectra.reshape(1, nb, 2, nf, pts), power.reshape(1, nb, 2, nf, pts))


def solution(mesh):
    in_specs = (P("ta", "ga", None), P(), P())
    out_specs = (P("ga", None, None, None, "ta"), P("ga", None, None, None, "ta"))
    return jax.shard_map(shards, mesh=mesh, in_specs=in_specs, out_specs=out_specs, check_vma=False)
```

```python
import functools
import math

import jax
import jax.numpy as jnp
from jax import lax
from jax.experimental import pallas as pl
from jax.experimental.pallas import tpu as pltpu
from jax.sharding import PartitionSpec as P

NFFT = 256
POWER_TILES = 2
MESH = pl.DeviceIdType.MESH
F32 = jnp.float32
BF16 = jnp.bfloat16


def build_table(phase, freqs, table):
    nf, nfft = phase.shape
    sample = lax.broadcasted_iota(jnp.int32, (1, nfft), 1)

    def phase_row(j, carry):
        phase[pl.ds(j, 1), :] = (freqs[j] * sample) % nfft
        return carry

    lax.fori_loop(0, nf, phase_row, 0)
    angle_val = 2.0 * math.pi / nfft * phase[...].astype(F32)
    window = 0.5 - 0.5 * jnp.cos(2.0 * math.pi / nfft * sample.astype(F32))
    norm_scale = 2.0 / math.sqrt(nfft)
    table[:nf, :] = (window * jnp.cos(angle_val) * norm_scale).astype(BF16)
    table[nf:, :] = (-window * jnp.sin(angle_val) * norm_scale).astype(BF16)


def round_up(value, step):
    return (value + step - 1) // step * step


def half_mask(nf, lanes):
    lane = lax.broadcasted_iota(jnp.int32, (8, lanes), 1)
    return lane % (2 * nf) < nf


def swap_halves(r, nf):
    lanes = r.shape[1]
    left = pltpu.roll(r, lanes - nf, 1)
    right = pltpu.roll(r, nf, 1)
    return jnp.where(half_mask(nf, lanes), left, right)


def diagonal(nf, lanes):
    row = lax.broadcasted_iota(jnp.int32, (nf, lanes), 0)
    lane = lax.broadcasted_iota(jnp.int32, (nf, lanes), 1)
    return lane % nf == row


def direct_plan(n, pts, chunks, x_ref, arrived, send_sem, recv_sem):
    me = lax.axis_index("ta")
    mz = lax.axis_index("ga")
    times = x_ref.shape[0]
    every = [(k, o) for k in range(len(chunks)) for o in range(1, n)]

    def piece(k, o):
        c0, cw = chunks[k]
        peer = lax.rem(me + o, n)
        return pltpu.make_async_remote_copy(
            src_ref=x_ref.at[:, pl.ds(pl.multiple_of(peer * pts + c0, 128), cw)],
            dst_ref=arrived.at[pl.ds(pl.multiple_of(me * times, times), times), pl.ds(c0, cw)],
            send_sem=send_sem.at[k, o],
            recv_sem=recv_sem.at[k, o],
            device_id=(peer, mz),
            device_id_type=MESH,
        )

    def begin():
        for k, o in every:
            piece(k, o).start()

    def follow():
        pass

    def receive(k):
        for o in range(1, n):
            piece(k, o).wait_recv()

    def finish():
        for k, o in every:
            piece(k, o).wait_send()

    return begin, follow, receive, finish


def square_plan(pts, chunks, x_ref, arrived, relay, send_sem, recv_sem):
    me = lax.axis_index("ta")
    mz = lax.axis_index("ga")
    times = x_ref.shape[0]
    core, x, y = me % 2, (me // 2) % 2, me // 4
    count = range(len(chunks))

    def index(yy, xx, cc):
        return (yy * 2 + xx) * 2 + cc

    def copy(k, src, dst, slot_out, slot_in, device):
        return pltpu.make_async_remote_copy(
            src_ref=src, dst_ref=dst, send_sem=send_sem.at[k, slot_out], recv_sem=recv_sem.at[k, slot_in],
            device_id=(device, mz), device_id_type=MESH)

    def columns(k, owner):
        c0, cw = chunks[k]
        return x_ref.at[:, pl.ds(pl.multiple_of(owner * pts + c0, 128), cw)]

    def place(k, source):
        c0, cw = chunks[k]
        return arrived.at[pl.ds(pl.multiple_of(source * times, times), times), pl.ds(c0, cw)]

    def to_relay(k, c):
        c0, cw = chunks[k]
        return copy(k, columns(k, index(1 - y, 1 - x, c)), relay.at[c, :, pl.ds(c0, cw)],
                    c, c, index(y, 1 - x, core))

    def along_x(k, c):
        peer = index(y, 1 - x, c)
        return copy(k, columns(k, peer), place(k, me), 2 + c, 2 + core, peer)

    def along_y(k, c):
        peer = index(1 - y, x, c)
        return copy(k, columns(k, peer), place(k, me), 4 + c, 4 + core, peer)

    def onward(k, c):
        c0, cw = chunks[k]
        return copy(k, relay.at[c, :, pl.ds(c0, cw)], place(k, index(y, 1 - x, core)),
                    7 + c, 7 + core, index(1 - y, x, c))

    def across(k):
        peer = index(y, x, 1 - core)
        return copy(k, columns(k, peer), place(k, me), 6, 6, peer)

    def arrival(k, slot):
        return copy(k, place(k, me), place(k, me), slot, slot, me)

    def begin():
        for k in count:
            for c in range(2):
                to_relay(k, c).start()
                along_y(k, c).start()
        for k in count:
            across(k).start()

    def follow():
        for k in count:
            for c in range(2):
                to_relay(k, c).wait_recv()
                onward(k, c).start()
            for c in range(2):
                along_x(k, c).start()

    def receive(k):
        across(k).wait_recv()
        for slot in (2, 3, 4, 5, 7, 8):
            arrival(k, slot).wait_recv()

    def finish():
        for k in count:
            for c in range(2):
                to_relay(k, c).wait_send()
                along_x(k, c).wait_send()
                along_y(k, c).wait_send()
                onward(k, c).wait_send()
            across(k).wait_send()

    return begin, follow, receive, finish


def exchange_kernel(dims, x_ref, starts_hbm, freqs_hbm, spec_ref, cross_ref,
                    starts_ref, freqs_ref, small_sem, phase, table_ref, arrived, w_ref, spec, gram, rows_a, rows_b, slots_ta, slots_ga,
                    send_sem, recv_sem, own_sem, out_sem, sa_sem, ra_sem, sb_sem, rb_sem, relay=None):
    n, nz, nb, nf, pts, chunks = dims
    me = lax.axis_index("ta")
    mz = lax.axis_index("ga")
    times = x_ref.shape[0]
    rows = nb * 2 * nf
    order = list(range(1, n))

    barrier = pltpu.get_barrier_semaphore()
    for o in order:
        pl.semaphore_signal(barrier, inc=1, device_id=(lax.rem(me + o, n), mz), device_id_type=MESH)
    for o in range(1, nz):
        pl.semaphore_signal(barrier, inc=1, device_id=(me, lax.rem(mz + o, nz)), device_id_type=MESH)
    pl.semaphore_wait(barrier, n - 1 + nz - 1)

    if relay is None:
        plan = direct_plan(n, pts, chunks, x_ref, arrived, send_sem, recv_sem)
    else:
        plan = square_plan(pts, chunks, x_ref, arrived, relay, send_sem, recv_sem)
    begin, follow, receive, finish = plan

    def own(k):
        c0, cw = chunks[k]
        src_col = pl.multiple_of(me * pts + c0, 128)
        dst_row = pl.multiple_of(me * times, times)
        return pltpu.make_async_copy(
            x_ref.at[:, pl.ds(src_col, cw)],
            arrived.at[pl.ds(dst_row, times), pl.ds(c0, cw)],
            own_sem.at[k],
        )

    begin()
    for k in range(len(chunks)):
        own(k).start()

    fetch_starts = pltpu.make_async_copy(starts_hbm, starts_ref, small_sem.at[0])
    fetch_freqs = pltpu.make_async_copy(freqs_hbm, freqs_ref, small_sem.at[1])
    fetch_starts.start()
    fetch_freqs.start()
    fetch_starts.wait()
    fetch_freqs.wait()
    build_table(phase, freqs_ref, table_ref)

    total_times = n * times
    lag = (lax.broadcasted_iota(jnp.int32, (NFFT, total_times), 1)
           - lax.broadcasted_iota(jnp.int32, (NFFT, total_times), 0))

    def build(b, carry):
        shift = jnp.where(lag == starts_ref[b], 1.0, 0.0).astype(BF16)
        placed = jnp.dot(table_ref[...], shift, preferred_element_type=F32)
        w_ref[pl.ds(pl.multiple_of(b * 2 * nf, 2 * nf), 2 * nf), :] = placed.astype(BF16)
        return carry

    lax.fori_loop(0, nb, build, 0)
    gram[...] = jnp.zeros_like(gram)
    rows_a[...] = jnp.zeros_like(rows_a)
    rows_b[...] = jnp.zeros_like(rows_b)

    follow()

    def out_copy(k):
        c0, cw = chunks[k]
        return pltpu.make_async_copy(
            spec.at[:, pl.ds(c0, cw)], spec_ref.at[:, pl.ds(c0, cw)], out_sem.at[k])

    for k, (c0, cw) in enumerate(chunks):
        own(k).wait()
        receive(k)
        s = jnp.dot(w_ref[...], arrived[:, c0:c0 + cw], preferred_element_type=F32).astype(BF16)
        spec[:, c0:c0 + cw] = s
        out_copy(k).start()
        gram[:, :rows] += lax.dot_general(
            s, s, (((1,), (1,)), ((), ())), preferred_element_type=F32)

    lanes = gram.shape[1]
    keep = diagonal(nf, lanes)
    for b in range(nb):
        top = gram[2 * b * nf:(2 * b + 1) * nf, :]
        low = gram[(2 * b + 1) * nf:(2 * b + 2) * nf, :]
        rows_a[b:b + 1, :] = jnp.sum(jnp.where(keep, top, 0.0), axis=0, keepdims=True)
        rows_b[b:b + 1, :] = jnp.sum(jnp.where(keep, low, 0.0), axis=0, keepdims=True)
    swapped = swap_halves(rows_b[...], nf)
    local = rows_a[...] + jnp.where(half_mask(nf, lanes), swapped, -swapped)

    slots_ta[me] = local.astype(BF16)

    def stage_a(o):
        peer = lax.rem(me + o, n)
        return pltpu.make_async_remote_copy(
            src_ref=slots_ta.at[me], dst_ref=slots_ta.at[me],
            send_sem=sa_sem.at[o], recv_sem=ra_sem.at[o],
            device_id=(peer, mz), device_id_type=MESH)

    def stage_b(o):
        peer = lax.rem(mz + o, nz)
        return pltpu.make_async_remote_copy(
            src_ref=slots_ga.at[mz], dst_ref=slots_ga.at[mz],
            send_sem=sb_sem.at[o], recv_sem=rb_sem.at[o],
            device_id=(me, peer), device_id_type=MESH)

    for o in order:
        stage_a(o).start()
    for o in order:
        stage_a(o).wait_recv()
    plane = slots_ta[0].astype(F32)
    for i in range(1, n):
        plane = plane + slots_ta[i].astype(F32)
    slots_ga[mz] = plane.astype(BF16)
    for o in range(1, nz):
        stage_b(o).start()
    for o in range(1, nz):
        stage_b(o).wait_recv()
    whole = slots_ga[0].astype(F32)
    for i in range(1, nz):
        whole = whole + slots_ga[i].astype(F32)
    cross_ref[...] = whole

    for k in range(len(chunks)):
        out_copy(k).wait()
    finish()
    for o in order:
        stage_a(o).wait_send()
    for o in range(1, nz):
        stage_b(o).wait_send()


def power_kernel(dims, scale, cross_ref, spec_ref, spec_out, power_out, mix, result, spec_sem, tile_sem):
    nb, nf, tile = dims
    rows, pts = spec_ref.shape
    lanes = cross_ref.shape[1]
    spectra_copy = pltpu.make_async_copy(spec_ref, spec_out, spec_sem)
    spectra_copy.start()
    cross = cross_ref[...] * scale
    swapped = swap_halves(cross, nf)
    turned = jnp.where(half_mask(nf, lanes), -swapped, swapped)
    keep = diagonal(nf, lanes)
    for b in range(nb):
        for c, source in enumerate((cross, turned)):
            m = jnp.where(keep, jnp.broadcast_to(source[b:b + 1, :], (nf, lanes)), 0.0)[:, :rows]
            r0 = (2 * b + c) * nf
            mix[r0:r0 + nf, :] = m.astype(BF16)

    def tile_copy(i):
        part = pl.ds(i * tile, tile)
        return pltpu.make_async_copy(result.at[:, part], power_out.at[:, part], tile_sem.at[i])

    for i in range(pts // tile):
        result[:, i * tile:(i + 1) * tile] = jnp.dot(
            mix[...], spec_ref[:, i * tile:(i + 1) * tile], preferred_element_type=F32)
        tile_copy(i).start()
    for i in range(pts // tile):
        tile_copy(i).wait()
    spectra_copy.wait()


def shards(snapshots, block_starts, kept_freqs):
    n = lax.axis_size("ta")
    nz = lax.axis_size("ga")
    nb = block_starts.shape[0]
    nf = kept_freqs.shape[0]
    times = snapshots.shape[0]
    pts = snapshots.shape[2] // n
    rows = nb * 2 * nf
    lanes = round_up(rows, 128)
    assert nb <= 8
    square = n == 8
    width = pts // 8
    chunks = [(0, 2 * width), (2 * width, 2 * width), (4 * width, 2 * width), (6 * width, 2 * width)]
    nk = len(chunks)
    operands = [pltpu.with_memory_space_constraint(a, pltpu.HBM) for a in (
        snapshots.reshape(times, snapshots.shape[2]), block_starts, kept_freqs)]
    dma = pltpu.SemaphoreType.DMA
    spectra, cross = pl.pallas_call(
        functools.partial(exchange_kernel, (n, nz, nb, nf, pts, chunks)),
        out_shape=(jax.ShapeDtypeStruct((rows, pts), BF16),
                   jax.ShapeDtypeStruct((8, lanes), F32)),
        in_specs=[pl.BlockSpec(memory_space=pl.ANY)] * 3,
        out_specs=(pl.BlockSpec(memory_space=pl.ANY), pl.BlockSpec(memory_space=pltpu.VMEM)),
        scratch_shapes=[
            pltpu.SMEM((nb,), jnp.int32),
            pltpu.SMEM((nf,), jnp.int32),
            dma((2,)),
            pltpu.VMEM((nf, NFFT), jnp.int32),
            pltpu.VMEM((2 * nf, NFFT), BF16),
            pltpu.VMEM((n * times, pts), BF16),
            pltpu.VMEM((rows, n * times), BF16),
            pltpu.VMEM((rows, pts), BF16),
            pltpu.VMEM((rows, lanes), F32),
            pltpu.VMEM((8, lanes), F32),
            pltpu.VMEM((8, lanes), F32),
            pltpu.VMEM((n, 8, lanes), BF16),
            pltpu.VMEM((nz, 8, lanes), BF16),
            dma((nk, max(n, 9))), dma((nk, max(n, 9))), dma((nk,)), dma((nk,)),
            dma((n,)), dma((n,)), dma((nz,)), dma((nz,)),
        ] + ([pltpu.VMEM((2, times, pts), BF16)] if square else []),
        compiler_params=pltpu.CompilerParams(
            collective_id=0, has_side_effects=True, vmem_limit_bytes=40 * 1024 * 1024),
        name="exchange",
    )(*operands)

    tile = pts // POWER_TILES
    spectra, power = pl.pallas_call(
        functools.partial(power_kernel, (nb, nf, tile), 1.0 / float(nb * pts * n * nz)),
        out_shape=(jax.ShapeDtypeStruct((rows, pts), BF16),
                   jax.ShapeDtypeStruct((rows, pts), F32)),
        in_specs=[pl.BlockSpec(memory_space=pltpu.VMEM)] * 2,
        out_specs=(pl.BlockSpec(memory_space=pltpu.HBM), pl.BlockSpec(memory_space=pltpu.HBM)),
        scratch_shapes=[pltpu.VMEM((rows, rows), BF16), pltpu.VMEM((rows, pts), F32),
                        dma(()), dma((pts // tile,))],
        compiler_params=pltpu.CompilerParams(vmem_limit_bytes=32 * 1024 * 1024),
        name="power",
    )(cross, spectra)
    return (spectra.reshape(1, nb, 2, nf, pts), power.reshape(1, nb, 2, nf, pts))


def solution(mesh):
    in_specs = (P("ta", "ga", None), P(), P())
    out_specs = (P("ga", None, None, None, "ta"), P("ga", None, None, None, "ta"))
    return jax.shard_map(shards, mesh=mesh, in_specs=in_specs, out_specs=out_specs, check_vma=False)
```
